32 devices in a mesh: lat: 4 (over z), lon: 8 (over y, x, core).
Axes of the slice: x: 2, y: 2, z: 4, core: 2. Of those that a mesh axis runs over, the one named last changes fastest.
Arguments:
- latent: bfloat16 [48, 576, 512], P('lat', 'lon'), may hold values from -1000 to 1000
- w_qkv: bfloat16 [512, 1536], replicated, may hold values from -1 to 1
- w_proj: bfloat16 [512, 512], replicated, may hold values from -0.25 to 0.25
- w_fc1: bfloat16 [512, 2048], replicated, may hold values from -0.25 to 0.25
- w_fc2: bfloat16 [2048, 512], replicated, may hold values from -0.125 to 0.125
- w_head: bfloat16 [512, 1024], replicated, may hold values from -4 to 4
- target_bins: int32 [48, 576, 4], P('lat', 'lon'), may hold values from 0 to 255
- land_mask: int32 [48, 576], P('lat', 'lon'), may hold values 0 or 1
Outputs:
- grad_latent: bfloat16 [48, 576, 512], P('lat', 'lon')
- grad_qkv: float32 [512, 1536], P(('lat', 'lon'))
- grad_proj: float32 [512, 512], P(('lat', 'lon'))
- grad_fc1: float32 [512, 2048], P(('lat', 'lon'))
- grad_fc2: float32 [2048, 512], P(('lat', 'lon'))
- grad_head: float32 [512, 1024], P(('lat', 'lon'))
The draws below stay inside these ranges and needn't reach their ends.
All inputs are finite; a program needn't handle non-finite values. No bound on the sum of `land_mask` on one device may be relied on, other than what follows from the above.
Results may differ from the reference program's by a relative error of at most 0.015.
Values may be sent and summed in bfloat16 or wider, within the bound.
A program may use at most 128 MiB of HBM per device.

```python
import math
import jax
import jax.numpy as jnp
from jax import lax

D = 512
HEADS = 8
FF = 2048
BINS = 256
VARS = 4
WIN_LAT = 6
WIN_LON = 12
HEAD_DIM = 64
NLAT = 48
NLON = 576


def draw_latent(key, part):
    key_noise, key_scale, key_other = jax.random.split(jax.random.fold_in(key, 1), 3)
    noise_vals = jax.random.normal(key_noise, (NLAT, NLON, D), jnp.float32)
    token_scale = jnp.exp(jax.random.uniform(key_scale, (NLAT, NLON, 1), jnp.float32, 0.0, math.log(10.0)))
    feature_scale = jnp.exp(jax.random.uniform(key_other, (D,), jnp.float32, 0.0, math.log(10.0)))
    values_out = token_scale * feature_scale * noise_vals
    return jnp.clip(values_out, -1000.0, 1000.0).astype(jnp.bfloat16)


def draw_w_qkv(key, part):
    base_vals = jax.random.normal(jax.random.fold_in(key, 2), (D, 3 * D), jnp.float32) / math.sqrt(D)
    return jnp.clip(base_vals, -1.0, 1.0).astype(jnp.bfloat16)


def draw_w_head(key, part):
    base_vals = jax.random.normal(jax.random.fold_in(key, 4), (D, VARS * BINS), jnp.float32) * (3.0 / math.sqrt(D))
    return jnp.clip(base_vals, -4.0, 4.0).astype(jnp.bfloat16)


def plant(entries, stream_key, least, largest):
    dims = entries.shape
    index_at = [jax.random.randint(jax.random.fold_in(stream_key, axis), (), 0, dims[axis]) for axis in range(len(dims))]
    entries = entries.at[tuple(index_at)].set(least)
    longest = dims.index(max(dims))
    index_at[longest] = (index_at[longest] + 1) % dims[longest]
    return entries.at[tuple(index_at)].set(largest)


def noise(stream_key, dims, spread, most, kind=jnp.bfloat16):
    return jnp.clip(spread * jax.random.normal(stream_key, dims, jnp.float32), -most, most).astype(kind)


def setup_inputs(seed: int = 0) -> dict:
    key_of = jax.random.split(jax.random.key(seed), 9)
    latent = draw_latent(jax.random.fold_in(key_of[8], 71), 0)
    w_qkv = draw_w_qkv(jax.random.fold_in(key_of[8], 71), 0)
    w_proj = noise(key_of[2], (D, D), D ** -0.5, 0.25)
    w_fc1 = noise(key_of[3], (D, FF), D ** -0.5, 0.25)
    w_fc2 = noise(key_of[4], (FF, D), FF ** -0.5, 0.125)
    w_head = draw_w_head(jax.random.fold_in(key_of[8], 71), 0)
    target_bins = plant(jax.random.randint(key_of[6], (NLAT, NLON, VARS), 0, BINS), jax.random.fold_in(key_of[6], 1), 0, BINS - 1).astype(jnp.int32)
    land_mask = plant((jax.random.randint(key_of[7], (NLAT, NLON), 0, 4) < 3).astype(jnp.int32), jax.random.fold_in(key_of[7], 1), 0, 1)
    return dict(latent=latent, w_qkv=w_qkv, w_proj=w_proj, w_fc1=w_fc1, w_fc2=w_fc2, w_head=w_head, target_bins=target_bins, land_mask=land_mask)


eps = 1e-05
smear = 0.75
masked = -1e+30

def normalize(values_in):
    centre = lax.optimization_barrier(jnp.mean(values_in, -1, keepdims=True))
    offset = values_in - centre
    inverse = lax.rsqrt(lax.optimization_barrier(jnp.mean(offset * offset, -1, keepdims=True)) + eps)
    return (offset * inverse, inverse)

def norm_back(scaled, inverse, upstream):
    return inverse * (upstream - lax.optimization_barrier(jnp.mean(upstream, -1, keepdims=True)) - scaled * lax.optimization_barrier(jnp.mean(upstream * scaled, -1, keepdims=True)))

def gelu_parts(pre_act):
    normal_cdf = 0.5 * (1.0 + jax.scipy.special.erf(pre_act / math.sqrt(2.0)))
    density = jnp.exp(-0.5 * pre_act * pre_act) / math.sqrt(2.0 * math.pi)
    return (pre_act * normal_cdf, normal_cdf + pre_act * density)

def mixing(form, left, right):
    return jnp.einsum(form, left.astype(jnp.float32), right.astype(jnp.float32))

def to_windows(block):
    row_count, col_count, feat_count = block.shape
    shaped = block.reshape(row_count // WIN_LAT, WIN_LAT, col_count // WIN_LON, WIN_LON, feat_count)
    return shaped.transpose(0, 2, 1, 3, 4).reshape(-1, WIN_LAT * WIN_LON, feat_count)

def from_windows(packed, row_count, col_count):
    feat_count = packed.shape[-1]
    shaped = packed.reshape(row_count // WIN_LAT, col_count // WIN_LON, WIN_LAT, WIN_LON, feat_count)
    return shaped.transpose(0, 2, 1, 3, 4).reshape(row_count, col_count, feat_count)

def window_setup(qkv_all, row_labels):
    row_count, col_count, _ = qkv_all.shape
    packed = to_windows(qkv_all)
    heads_view = packed.reshape(packed.shape[0], packed.shape[1], 3, HEADS, HEAD_DIM)
    window_tags = to_windows(jnp.broadcast_to(row_labels[:, None, None], (row_count, col_count, 1)))[:, :, 0]
    allowed = window_tags[:, :, None] == window_tags[:, None, :]
    scores = mixing('wqhd,wkhd->whqk', heads_view[:, :, 0], heads_view[:, :, 1]) * HEAD_DIM ** (-0.5)
    scores = jnp.where(allowed[:, None], scores, masked)
    highest = lax.optimization_barrier(jnp.max(scores, -1, keepdims=True))
    exponent = jnp.exp(scores - highest)
    return (heads_view, exponent / lax.optimization_barrier(jnp.sum(exponent, -1, keepdims=True)))

def window_forward(heads_view, attn_probs, row_count, col_count):
    context = mixing('whqk,wkhd->wqhd', attn_probs.astype(jnp.bfloat16), heads_view[:, :, 2]).astype(jnp.bfloat16)
    return from_windows(context.reshape(context.shape[0], context.shape[1], -1), row_count, col_count)

def window_backward(heads_view, attn_probs, d_context, row_count, col_count):
    probs_low = attn_probs.astype(jnp.bfloat16)
    upstream = to_windows(d_context).reshape(heads_view.shape[0], heads_view.shape[1], HEADS, HEAD_DIM)
    d_probs = mixing('wqhd,wkhd->whqk', upstream, heads_view[:, :, 2])
    d_value = mixing('whqk,wqhd->wkhd', probs_low, upstream)
    d_scores = attn_probs * (d_probs - lax.optimization_barrier(jnp.sum(d_probs * attn_probs, -1, keepdims=True))) * HEAD_DIM ** (-0.5)
    d_scores = d_scores.astype(jnp.bfloat16)
    d_query = mixing('whqk,wkhd->wqhd', d_scores, heads_view[:, :, 1])
    d_key = mixing('whqk,wqhd->wkhd', d_scores, heads_view[:, :, 0])
    joined = jnp.stack([d_query, d_key, d_value], 2).astype(jnp.bfloat16)
    return from_windows(joined.reshape(joined.shape[0], joined.shape[1], -1), row_count, col_count)

def hl_target(bin_index):
    bin_edges = jnp.arange(BINS + 1, dtype=jnp.int32).astype(jnp.float32)
    centre = bin_index.astype(jnp.float32)[..., None] + 0.5
    cumulative = 0.5 * jax.scipy.special.erf((bin_edges - centre) / (smear * math.sqrt(2.0)))
    return (cumulative[..., 1:] - cumulative[..., :-1]) / (cumulative[..., -1:] - cumulative[..., :1])

def head_grad(normed3, w_head, target_bins, land_mask):
    logits = jnp.dot(normed3, w_head, preferred_element_type=jnp.float32).reshape(-1, VARS, BINS)
    highest = lax.optimization_barrier(jnp.max(logits, -1, keepdims=True))
    exponent = jnp.exp(logits - highest)
    bin_probs = exponent / lax.optimization_barrier(jnp.sum(exponent, -1, keepdims=True))
    weight_tok = land_mask.reshape(-1).astype(jnp.float32)[:, None, None] / VARS
    d_logits = weight_tok * (bin_probs - hl_target(target_bins.reshape(-1, VARS)))
    return d_logits.astype(jnp.bfloat16).reshape(-1, VARS * BINS)

def reference(latent, w_qkv, w_proj, w_fc1, w_fc2, w_head, target_bins, land_mask):
    half_rows = WIN_LAT // 2
    half_cols = WIN_LON // 2
    feat_width = latent.shape[-1]
    residual_in = latent.astype(jnp.float32)
    scaled1, inverse1 = normalize(residual_in)
    normed1 = scaled1.astype(jnp.bfloat16)
    shifted = jnp.roll(normed1, (-half_rows, -half_cols), (0, 1))
    qkv_all = jnp.dot(shifted.reshape(-1, feat_width), w_qkv, preferred_element_type=jnp.float32).astype(jnp.bfloat16)
    qkv_rows = qkv_all.reshape(NLAT // WIN_LAT, WIN_LAT, NLON, 3 * feat_width)
    row_labels = (jnp.arange(NLAT, dtype=jnp.int32) + half_rows >= NLAT).astype(jnp.int32)
    label_rows = row_labels.reshape(NLAT // WIN_LAT, WIN_LAT)

    def context_rows(packed_in):
        heads_view, attn_probs = window_setup(packed_in[0], packed_in[1])
        return window_forward(heads_view, attn_probs, WIN_LAT, NLON)
    context = lax.map(context_rows, (qkv_rows, label_rows)).reshape(-1, feat_width)
    attended = jnp.dot(context, w_proj, preferred_element_type=jnp.float32).astype(jnp.bfloat16)
    attended = jnp.roll(attended.reshape(NLAT, NLON, feat_width), (half_rows, half_cols), (0, 1))
    attended = lax.optimization_barrier(attended)
    residual = residual_in + attended.astype(jnp.float32)
    scaled2, inverse2 = normalize(residual)
    normed2 = scaled2.astype(jnp.bfloat16).reshape(-1, feat_width)
    pre_act = jnp.dot(normed2, w_fc1, preferred_element_type=jnp.float32)
    activated, gelu_slope = gelu_parts(pre_act)
    activated = activated.astype(jnp.bfloat16)
    block_out = residual + jnp.dot(activated, w_fc2, preferred_element_type=jnp.float32).reshape(NLAT, NLON, feat_width)
    scaled3, inverse3 = normalize(block_out)
    normed3 = scaled3.astype(jnp.bfloat16).reshape(-1, feat_width)
    d_logits = head_grad(normed3, w_head, target_bins, land_mask)
    grad_head = jnp.dot(normed3.T, d_logits, preferred_element_type=jnp.float32)
    d_out = norm_back(scaled3, inverse3, jnp.dot(d_logits, w_head.T, preferred_element_type=jnp.float32).reshape(NLAT, NLON, feat_width))
    d_outb = d_out.astype(jnp.bfloat16).reshape(-1, feat_width)
    grad_fc2 = jnp.dot(activated.T, d_outb, preferred_element_type=jnp.float32)
    d_pre = (jnp.dot(d_outb, w_fc2.T, preferred_element_type=jnp.float32) * gelu_slope).astype(jnp.bfloat16)
    grad_fc1 = jnp.dot(normed2.T, d_pre, preferred_element_type=jnp.float32)
    d_resid = d_out + norm_back(scaled2, inverse2, jnp.dot(d_pre, w_fc1.T, preferred_element_type=jnp.float32).reshape(NLAT, NLON, feat_width))
    d_attended = jnp.roll(d_resid.astype(jnp.bfloat16), (-half_rows, -half_cols), (0, 1)).reshape(-1, feat_width)
    grad_proj = jnp.dot(context.T, d_attended, preferred_element_type=jnp.float32)
    d_context = jnp.dot(d_attended, w_proj.T, preferred_element_type=jnp.float32).astype(jnp.bfloat16)
    d_context_rows = d_context.reshape(NLAT // WIN_LAT, WIN_LAT, NLON, feat_width)

    def gradient_rows(packed_in):
        heads_view, attn_probs = window_setup(packed_in[0], packed_in[1])
        return window_backward(heads_view, attn_probs, packed_in[2], WIN_LAT, NLON)
    d_qkv = lax.map(gradient_rows, (qkv_rows, label_rows, d_context_rows)).reshape(-1, 3 * feat_width)
    grad_qkv = jnp.dot(shifted.reshape(-1, feat_width).T, d_qkv, preferred_element_type=jnp.float32)
    d_shifted = jnp.dot(d_qkv, w_qkv.T, preferred_element_type=jnp.float32).astype(jnp.bfloat16)
    d_shifted = jnp.roll(d_shifted.reshape(NLAT, NLON, feat_width), (half_rows, half_cols), (0, 1))
    d_shifted = lax.optimization_barrier(d_shifted)
    grad_latent = (d_resid + norm_back(scaled1, inverse1, d_shifted.astype(jnp.float32))).astype(jnp.bfloat16)
    return (grad_latent, grad_qkv, grad_proj, grad_fc1, grad_fc2, grad_head)
```

```python
import math

import jax
import jax.numpy as jnp
from jax import lax
from jax.experimental import pallas as pl
from jax.experimental.pallas import tpu as pltpu
from jax.sharding import PartitionSpec as P

HEADS = 8
BINS = 256
VARS = 4
WIN_LAT = 6
WIN_LON = 12
HEAD_DIM = 64


eps = 1e-05
smear = 0.75
masked = -1e30


def shifted_2(value, axis, steps):
    count = lax.axis_size(axis)
    pairs = [(source, (source + steps) % count) for source in range(count)]
    return lax.ppermute(value, axis, pairs)


def normalize(values_in):
    centre = jnp.mean(values_in, -1, keepdims=True)
    offset = values_in - centre
    inverse = lax.rsqrt(jnp.mean(offset * offset, -1, keepdims=True) + eps)
    return (offset * inverse, inverse)


def norm_back(scaled, inverse, upstream):
    return inverse * (
        upstream
        - jnp.mean(upstream, -1, keepdims=True)
        - scaled * jnp.mean(upstream * scaled, -1, keepdims=True)
    )


def gelu_parts(pre_act):
    normal_cdf = 0.5 * (1.0 + jax.scipy.special.erf(pre_act / math.sqrt(2.0)))
    density = jnp.exp(-0.5 * pre_act * pre_act) / math.sqrt(2.0 * math.pi)
    return (pre_act * normal_cdf, normal_cdf + pre_act * density)


def dot_over(left, right, left_dim, right_dim):
    return lax.dot_general(
        left, right, (((left_dim,), (right_dim,)), ((), ())), preferred_element_type=jnp.float32
    )


def to_windows(block):
    row_count, col_count, feat_count = block.shape
    shaped = block.reshape(row_count // WIN_LAT, WIN_LAT, col_count // WIN_LON, WIN_LON, feat_count)
    return shaped.transpose(0, 2, 1, 3, 4).reshape(-1, feat_count)


def from_windows(packed, row_count, col_count):
    feat_count = packed.shape[-1]
    shaped = packed.reshape(
        row_count // WIN_LAT, col_count // WIN_LON, WIN_LAT, WIN_LON, feat_count
    )
    return shaped.transpose(0, 2, 1, 3, 4).reshape(row_count, col_count, feat_count)


def head_part(ref, part, head, width):
    start = part * width + head * HEAD_DIM
    return ref[0, :, start : start + HEAD_DIM]


def attention_kernel(qkv_ref, allowed_ref, context_ref, probs_ref):
    width = context_ref.shape[-1]
    allowed = allowed_ref[0] > 0.5
    pieces = []
    for head in range(HEADS):
        query = head_part(qkv_ref, 0, head, width)
        key = head_part(qkv_ref, 1, head, width)
        value = head_part(qkv_ref, 2, head, width)
        scores = dot_over(query, key, 1, 1) * HEAD_DIM ** (-0.5)
        scores = jnp.where(allowed, scores, masked)
        exponent = jnp.exp(scores - jnp.max(scores, -1, keepdims=True))
        probs = exponent / jnp.sum(exponent, -1, keepdims=True)
        probs_ref[0, head] = probs
        pieces.append(dot_over(probs.astype(jnp.bfloat16), value, 1, 0))
    context_ref[0] = jnp.concatenate(pieces, -1).astype(jnp.bfloat16)


def attention_back_kernel(qkv_ref, probs_ref, d_context_ref, d_qkv_ref):
    width = d_context_ref.shape[-1]
    d_queries, d_keys, d_values = [], [], []
    for head in range(HEADS):
        query = head_part(qkv_ref, 0, head, width)
        key = head_part(qkv_ref, 1, head, width)
        value = head_part(qkv_ref, 2, head, width)
        upstream = head_part(d_context_ref, 0, head, width)
        probs = probs_ref[0, head]
        d_probs = dot_over(upstream, value, 1, 1)
        d_scores = (
            probs
            * (d_probs - jnp.sum(d_probs * probs, -1, keepdims=True))
            * HEAD_DIM ** (-0.5)
        )
        d_scores_t = d_scores.T.astype(jnp.bfloat16)
        d_scores = d_scores.astype(jnp.bfloat16)
        d_queries.append(dot_over(d_scores, key, 1, 0))
        d_keys.append(dot_over(d_scores_t, query, 1, 0))
        d_values.append(dot_over(probs.T.astype(jnp.bfloat16), upstream, 1, 0))
    for part, pieces in enumerate((d_queries, d_keys, d_values)):
        joined = jnp.concatenate(pieces, -1).astype(jnp.bfloat16)
        d_qkv_ref[0, :, part * width : (part + 1) * width] = joined


def whole_block(*dims):
    return pl.BlockSpec((1, *dims), lambda place: (place,) + (0,) * len(dims))


def attention(qkv_all, allowed, windows_across):
    windows, tokens, triple = qkv_all.shape
    width = triple // 3
    return pl.pallas_call(
        attention_kernel,
        grid=(windows,),
        in_specs=[
            whole_block(tokens, triple),
            pl.BlockSpec((1, tokens, tokens), lambda place: (place // windows_across, 0, 0)),
        ],
        out_specs=[whole_block(tokens, width), whole_block(HEADS, tokens, tokens)],
        out_shape=[
            jax.ShapeDtypeStruct((windows, tokens, width), jnp.bfloat16),
            jax.ShapeDtypeStruct((windows, HEADS, tokens, tokens), jnp.float32),
        ],
        cost_estimate=pl.CostEstimate(
            flops=4 * windows * tokens * tokens * width * 20, bytes_accessed=8000000, transcendentals=0
        ),
        name="attention",
    )(qkv_all, allowed)


def attention_back(qkv_all, probs, d_context):
    windows, tokens, triple = qkv_all.shape
    width = triple // 3
    return pl.pallas_call(
        attention_back_kernel,
        grid=(windows,),
        in_specs=[
            whole_block(tokens, triple),
            whole_block(HEADS, tokens, tokens),
            whole_block(tokens, width),
        ],
        out_specs=whole_block(tokens, triple),
        out_shape=jax.ShapeDtypeStruct((windows, tokens, triple), jnp.bfloat16),
        cost_estimate=pl.CostEstimate(
            flops=8 * windows * tokens * tokens * width * 20, bytes_accessed=10000000, transcendentals=0
        ),
        name="attention_back",
    )(qkv_all, probs, d_context)


def target_table():
    edges = jnp.arange(BINS + 1, dtype=jnp.int32).astype(jnp.float32)
    centre = jnp.arange(BINS, dtype=jnp.int32).astype(jnp.float32)[:, None] + 0.5
    cumulative = 0.5 * jax.scipy.special.erf((edges - centre) / (smear * math.sqrt(2.0)))
    table = (cumulative[:, 1:] - cumulative[:, :-1]) / (cumulative[:, -1:] - cumulative[:, :1])
    upper = lax.reduce_precision(table, 8, 7)
    lower = (table - upper).astype(jnp.bfloat16)
    return (upper.astype(jnp.bfloat16), lower)


def head_grad(normed3, w_head, target_bins, land_mask):
    upper, lower = target_table()
    weight_tok = land_mask.astype(jnp.float32) / VARS
    bins = jnp.arange(BINS, dtype=jnp.int32)[None, :]
    pieces = []
    for var in range(VARS):
        logits = jnp.dot(
            normed3,
            w_head[:, var * BINS : (var + 1) * BINS],
            preferred_element_type=jnp.float32,
        )
        exponent = jnp.exp(logits - jnp.max(logits, -1, keepdims=True))
        bin_probs = exponent / jnp.sum(exponent, -1, keepdims=True)
        picked = (target_bins[:, var : var + 1] == bins).astype(jnp.bfloat16)
        target = jnp.dot(picked, upper, preferred_element_type=jnp.float32) + jnp.dot(
            picked, lower, preferred_element_type=jnp.float32
        )
        pieces.append((weight_tok * (bin_probs - target)).astype(jnp.bfloat16))
    return jnp.concatenate(pieces, 1)


def roll_ahead(block):
    half_rows = WIN_LAT // 2
    half_cols = WIN_LON // 2
    edge_cols = shifted_2(block[:, :half_cols], "lon", -1)
    moved_cols = jnp.concatenate([block[:, half_cols:], edge_cols], 1)
    edge_rows = shifted_2(moved_cols[:half_rows], "lat", -1)
    return jnp.concatenate([moved_cols[half_rows:], edge_rows], 0)


def roll_behind(block):
    half_rows = WIN_LAT // 2
    half_cols = WIN_LON // 2
    row_count, col_count = (block.shape[0], block.shape[1])
    edge_cols = shifted_2(block[:, col_count - half_cols :], "lon", 1)
    moved_cols = jnp.concatenate([edge_cols, block[:, : col_count - half_cols]], 1)
    edge_rows = shifted_2(moved_cols[row_count - half_rows :], "lat", 1)
    return jnp.concatenate([edge_rows, moved_cols[: row_count - half_rows]], 0)


def scatter_over(value, axis):
    return lax.psum_scatter(value, axis, scatter_dimension=0, tiled=True)


def local(latent, w_qkv, w_proj, w_fc1, w_fc2, w_head, target_bins, land_mask):
    row_count, col_count, feat_width = latent.shape
    half_rows = WIN_LAT // 2
    tokens = WIN_LAT * WIN_LON
    lat_total = row_count * lax.axis_size("lat")
    devices = lax.axis_size("lat") * lax.axis_size("lon")
    row_place = (
        lax.axis_index("lat") * row_count + jnp.arange(row_count, dtype=jnp.int32) + half_rows
    )
    row_labels = (row_place >= lat_total).astype(jnp.int32)
    window_tags = jnp.repeat(row_labels.reshape(-1, WIN_LAT), WIN_LON, axis=1)
    allowed = (window_tags[:, :, None] == window_tags[:, None, :]).astype(jnp.float32)
    marks = jnp.concatenate([target_bins, land_mask[:, :, None]], 2)
    residual_in = to_windows(roll_ahead(latent)).astype(jnp.float32)
    marks = to_windows(roll_ahead(marks))
    scaled1, inverse1 = normalize(residual_in)
    shifted = scaled1.astype(jnp.bfloat16)
    qkv_all = jnp.dot(shifted, w_qkv, preferred_element_type=jnp.float32).astype(jnp.bfloat16)
    qkv_all = qkv_all.reshape(-1, tokens, 3 * feat_width)
    context, attn_probs = attention(qkv_all, allowed, col_count // WIN_LON)
    context = context.reshape(-1, feat_width)
    attended = jnp.dot(context, w_proj, preferred_element_type=jnp.float32).astype(jnp.bfloat16)
    residual = residual_in + attended.astype(jnp.float32)
    scaled2, inverse2 = normalize(residual)
    normed2 = scaled2.astype(jnp.bfloat16)
    pre_act = jnp.dot(normed2, w_fc1, preferred_element_type=jnp.float32)
    activated, gelu_slope = gelu_parts(pre_act)
    activated = activated.astype(jnp.bfloat16)
    block_out = residual + jnp.dot(activated, w_fc2, preferred_element_type=jnp.float32)
    scaled3, inverse3 = normalize(block_out)
    normed3 = scaled3.astype(jnp.bfloat16)
    d_logits = head_grad(normed3, w_head, marks[:, :VARS], marks[:, VARS:])
    grad_head = jnp.dot(normed3.T, d_logits, preferred_element_type=jnp.float32)
    d_out = norm_back(
        scaled3, inverse3, jnp.dot(d_logits, w_head.T, preferred_element_type=jnp.float32)
    )
    d_outb = d_out.astype(jnp.bfloat16)
    grad_fc2 = jnp.dot(activated.T, d_outb, preferred_element_type=jnp.float32)
    d_pre = (jnp.dot(d_outb, w_fc2.T, preferred_element_type=jnp.float32) * gelu_slope).astype(
        jnp.bfloat16
    )
    grad_fc1 = jnp.dot(normed2.T, d_pre, preferred_element_type=jnp.float32)
    d_resid = d_out + norm_back(
        scaled2, inverse2, jnp.dot(d_pre, w_fc1.T, preferred_element_type=jnp.float32)
    )
    d_attended = d_resid.astype(jnp.bfloat16)
    grad_proj = jnp.dot(context.T, d_attended, preferred_element_type=jnp.float32)
    grads = [grad.astype(jnp.bfloat16) for grad in (grad_head, grad_fc1, grad_proj)]
    ratio = grad_fc2.shape[0] // feat_width
    low_fc2 = grad_fc2.astype(jnp.bfloat16).reshape(
        devices, ratio, feat_width // devices, feat_width
    )
    grads += [low_fc2[:, part].reshape(feat_width, feat_width) for part in range(ratio)]
    joined, d_attended = lax.optimization_barrier((jnp.concatenate(grads, 1), d_attended))
    early = scatter_over(joined, "lat")
    d_context = jnp.dot(d_attended, w_proj.T, preferred_element_type=jnp.float32).astype(
        jnp.bfloat16
    )
    d_qkv = attention_back(
        qkv_all, attn_probs, d_context.reshape(-1, tokens, feat_width)
    ).reshape(-1, 3 * feat_width)
    grad_qkv = jnp.dot(shifted.T, d_qkv, preferred_element_type=jnp.float32)
    late = scatter_over(grad_qkv.astype(jnp.bfloat16), "lat")
    summed = scatter_over(jnp.concatenate([late, early], 1), "lon").astype(jnp.float32)
    late, early = summed[:, : 3 * feat_width], summed[:, 3 * feat_width :]
    d_shifted = jnp.dot(d_qkv, w_qkv.T, preferred_element_type=jnp.float32).astype(jnp.bfloat16)
    grad_latent = (d_resid + norm_back(scaled1, inverse1, d_shifted.astype(jnp.float32))).astype(
        jnp.bfloat16
    )
    grad_latent = roll_behind(from_windows(grad_latent, row_count, col_count))
    cuts = [grad_head.shape[1], grad_fc1.shape[1], grad_proj.shape[1]]
    first, second, third = cuts[0], cuts[0] + cuts[1], sum(cuts)
    sum_fc2 = early[:, third:].reshape(-1, ratio, feat_width).transpose(1, 0, 2)
    return (
        grad_latent,
        late,
        early[:, second:third],
        early[:, first:second],
        sum_fc2.reshape(-1, feat_width),
        early[:, :first],
    )


def solution(mesh):
    placed = (
        P("lat", "lon", None),
        P(),
        P(),
        P(),
        P(),
        P(),
        P("lat", "lon", None),
        P("lat", "lon"),
    )
    return jax.shard_map(
        local,
        mesh=mesh,
        in_specs=placed,
        out_specs=(
            P("lat", "lon", None),
            P(("lat", "lon"), None),
            P(("lat", "lon"), None),
            P(("lat", "lon"), None),
            P(("lat", "lon"), None),
            P(("lat", "lon"), None),
        ),
        check_vma=False,
    )
```
